16 devices in a mesh: dp: 4 (over y, z, core), tp: 4 (over x).
Axes of the slice: x: 4, y: 2, z: 1, core: 2. Of those that a mesh axis runs over, the one named last changes fastest.
The devices are a block of a 4x4x8 slice.
Arguments:
- x: bfloat16 [5632, 3072], P(('dp', 'tp')), parts along dimension 0
- dy: bfloat16 [5632, 3072], P(('dp', 'tp')), parts along dimension 0
- pre: bfloat16 [5632, 9216], P('dp', 'tp'), parts along dimension 0
- w_in: bfloat16 [3072, 9216], P(None, 'tp')
- w_down: bfloat16 [9216, 3072], P('tp')
Outputs:
- output 1: bfloat16 [5632, 3072], P(('dp', 'tp')), parts along dimension 0
- output 2: bfloat16 [12288, 9216], P('dp', 'tp'), parts along dimension 0
- output 3: bfloat16 [36864, 3072], P(('dp', 'tp')), parts along dimension 0
There are 4 independent parts. The reference program is written for one: setup_inputs(seed, part) draws one part's arguments, and reference() takes and returns one part's arrays. A program takes and returns all parts, laid end to end along the dimension named above; an argument that names none is the same for every part.
All inputs are finite; a program needn't handle non-finite values.
Results may differ from the reference program's by a relative error of at most 0.012.
Values are sent between devices in bfloat16 or wider.
A program may use at most 768 MiB of HBM per device.

```python
import jax
import jax.numpy as jnp

ROWS = 1408
D = 3072
FF = 9216


def act(pre):
    return jnp.square(jax.nn.relu(pre))


def setup_inputs(seed: int = 0, part: int = 0) -> dict:
    kx, ky, ka, ki, kd = jax.random.split(jax.random.key(seed), 5)
    kx, ky, ka = (jax.random.fold_in(k, part) for k in (kx, ky, ka))
    drawn = {
        "x": jax.random.normal(kx, (ROWS, D), jnp.float32),
        "dy": jax.random.normal(ky, (ROWS, D), jnp.float32),
        "pre": jax.random.normal(ka, (ROWS, FF), jnp.float32),
        "w_in": jax.random.normal(ki, (D, FF), jnp.float32) * D**-0.5,
        "w_down": jax.random.normal(kd, (FF, D), jnp.float32) * FF**-0.5,
    }
    return {k: v.astype(jnp.bfloat16) for k, v in drawn.items()}


def reference(x, dy, pre, w_in, w_down):
    hidden, back = jax.vjp(act, pre.astype(jnp.float32))
    d_hidden = jnp.dot(dy, w_down.T, preferred_element_type=jnp.float32)
    d_pre = back(d_hidden)[0].astype(jnp.bfloat16)
    dx = jnp.dot(d_pre, w_in.T, preferred_element_type=jnp.float32)
    dw_in = jnp.dot(x.T, d_pre, preferred_element_type=jnp.float32)
    dw_down = jnp.dot(hidden.astype(jnp.bfloat16).T, dy, preferred_element_type=jnp.float32)
    return tuple(g.astype(jnp.bfloat16) for g in (dx, dw_in, dw_down))
```

```python
import jax
import jax.numpy as jnp
from jax import lax
from jax.sharding import PartitionSpec as P

CHUNKS = 2


def act(pre):
    return jnp.square(jax.nn.relu(pre))


def solution(mesh):
    n = mesh.shape["tp"]
    right = [(i, (i + 1) % n) for i in range(n)]
    left = [(i, (i - 1) % n) for i in range(n)]

    def send(a, ring):
        return lax.ppermute(a, "tp", ring)

    def step(x, dy, pre, w_in, w_down):
        me = lax.axis_index("tp")
        rows, d = x.shape
        half = rows // 2
        owner = [me, (me + n - 1) % n, (me + 1) % n, (me + 2) % n]

        def d_pre_of(block, who):
            p = lax.dynamic_slice_in_dim(pre, who * rows, rows, 0)
            _, back = jax.vjp(act, p.astype(jnp.float32))
            d_hidden = jnp.dot(block, w_down.T, preferred_element_type=jnp.float32)
            return back(d_hidden)[0].astype(jnp.bfloat16)

        def term_of(d_pre):
            return jnp.dot(d_pre, w_in.T, preferred_element_type=jnp.float32)

        dy_r, dy_l = send(dy, right), send(dy, left)
        x_r, x_l = send(x, right), send(x, left)
        dp0 = d_pre_of(dy, owner[0])
        t0 = term_of(dp0)
        dy_o = jnp.concatenate([send(dy_r[:half], right), send(dy_l[half:], left)])
        dp1 = d_pre_of(dy_r, owner[1])
        dp2 = d_pre_of(dy_l, owner[2])
        t1 = term_of(dp1)
        t2 = term_of(dp2)
        x_o = jnp.concatenate([send(x_r[:half], right), send(x_l[half:], left)])
        dp3 = d_pre_of(dy_o, owner[3])
        t3 = term_of(dp3)

        c = half // CHUNKS
        tops, bottoms = [], []
        for k in range(CHUNKS):
            a = slice(k * c, (k + 1) * c)
            b = slice(half + k * c, half + (k + 1) * c)
            s, u = t1[a].astype(jnp.bfloat16), t2[b].astype(jnp.bfloat16)
            for ta, tb in ((t3, t3), (t2, t1), (t0, t0)):
                s, u = send(s, right), send(u, left)
                s = (ta[a] + s.astype(jnp.float32)).astype(jnp.bfloat16)
                u = (tb[b] + u.astype(jnp.float32)).astype(jnp.bfloat16)
            tops.append(s)
            bottoms.append(u)
        dx = jnp.concatenate(tops + bottoms)

        def gather(parts):
            out = jnp.zeros((n * rows, parts[0].shape[1]), parts[0].dtype)
            for p, o in zip(parts, owner):
                out = lax.dynamic_update_slice_in_dim(out, p, o * rows, 0)
            return out

        dy_all = gather([dy, dy_r, dy_l, dy_o])
        hidden = act(pre.astype(jnp.float32)).astype(jnp.bfloat16)
        dw_down = jnp.einsum("ta,tb->ab", hidden, dy_all, preferred_element_type=jnp.float32).astype(jnp.bfloat16)
        x_all = gather([x, x_r, x_l, x_o])
        dp_all = gather([dp0, dp1, dp2, dp3])
        dw_in = jnp.einsum("ta,tb->ab", x_all, dp_all, preferred_element_type=jnp.float32).astype(jnp.bfloat16)
        return dx, dw_in, dw_down

    tokens, cols, both = P(("dp", "tp"), None), P("dp", "tp"), P(("dp", "tp"), None)
    return jax.shard_map(
        step,
        mesh=mesh,
        in_specs=(tokens, tokens, cols, P(None, "tp"), P("tp", None)),
        out_specs=(tokens, cols, both),
        check_vma=False,
    )
```

```python
import functools

import jax
import jax.numpy as jnp
from jax import lax
from jax.experimental import pallas as pl
from jax.experimental.pallas import tpu as pltpu
from jax.sharding import PartitionSpec as P

NT = (((1,), (1,)), ((), ()))
TN = (((0,), (0,)), ((), ()))
F32, BF16 = jnp.float32, jnp.bfloat16
TILE = 768
VMEM_LIMIT = 60 * 2**20


def act(pre):
    return jnp.square(jax.nn.relu(pre))


def backward_body(nd, pieces, blocks, chained, *refs):
    refs = refs[1 + chained:]
    dys, pres, (wd, wi), refs = refs[:pieces], refs[pieces:pieces + blocks], refs[pieces + blocks:pieces + blocks + 2], refs[pieces + blocks + 2:]
    dp_out, *t_out = refs[:2] if blocks == 1 else refs[:5]
    dp_all, *dy_all = refs[1 + len(t_out):]
    i = pl.program_id(0)
    rows = dp_out.shape[0] // blocks
    half = rows // 2
    tile = wd.shape[0]
    if pieces == 1:
        dy_all = dys[0]
    else:
        dy_all = dy_all[0]

        @pl.when(i == 0)
        def _():
            at = 0
            for dy in dys:
                dy_all[at:at + dy.shape[0]] = dy[...]
                at += dy.shape[0]

    @pl.when(i < nd)
    def _():
        d_hidden = lax.dot_general(dy_all[...], wd[...], NT, preferred_element_type=F32)
        for k in range(blocks):
            part = slice(k * rows, (k + 1) * rows)
            dp = (d_hidden[part] * (2.0 * jnp.maximum(pres[k][...].astype(F32), 0.0))).astype(BF16)
            dp_out[part] = dp
            dp_all[part, pl.ds(pl.multiple_of(i * tile, tile), tile)] = dp

    @pl.when(i >= nd)
    def _():
        t = lax.dot_general(dp_all[...], wi[...], NT, preferred_element_type=F32)
        if blocks == 1:
            t_out[0][...] = t
        else:
            first_a, first_b, rest_a, rest_b = t_out
            first_a[...] = t[:half].astype(BF16)
            rest_b[...] = t[half:rows]
            rest_a[...] = t[rows:rows + half]
            first_b[...] = t[rows + half:].astype(BF16)


def backward(dys, owners, pre, w_in, w_down, place, d_pre=None):
    chained = [] if d_pre is None else [d_pre]
    blocks = len(owners)
    total, d = sum(v.shape[0] for v in dys), dys[0].shape[1]
    rows, ff = total // blocks, pre.shape[1]
    half = rows // 2
    nd, ni = ff // TILE, d // TILE
    phase1 = lambda i: jnp.minimum(i, nd - 1)
    phase2 = lambda i: jnp.maximum(i - nd, 0)

    def pre_spec(k):
        return pl.BlockSpec((rows, TILE), lambda i, o: (o[k], phase1(i)))

    terms = [(rows, F32)] if blocks == 1 else [(half, BF16), (half, BF16), (half, F32), (half, F32)]
    return pl.pallas_call(
        functools.partial(backward_body, nd, len(dys), blocks, len(chained)),
        grid_spec=pltpu.PrefetchScalarGridSpec(
            num_scalar_prefetch=1,
            grid=(nd + ni,),
            in_specs=[pl.BlockSpec(memory_space=pl.ANY)] * len(chained)
            + [pl.BlockSpec(v.shape, lambda i, o: (0, 0)) for v in dys]
            + [pre_spec(k) for k in range(blocks)]
            + [pl.BlockSpec((TILE, d), lambda i, o: (phase1(i), 0)), pl.BlockSpec((TILE, ff), lambda i, o: (phase2(i), 0))],
            out_specs=[pl.BlockSpec((total, TILE), lambda i, o: (place, phase1(i)))]
            + [pl.BlockSpec((r, TILE), lambda i, o: (0, phase2(i))) for r, _ in terms],
            scratch_shapes=[pltpu.VMEM((total, ff), BF16)] + [pltpu.VMEM((total, d), BF16)] * (len(dys) > 1),
        ),
        out_shape=[jax.ShapeDtypeStruct((pre.shape[0], ff), BF16)] + [jax.ShapeDtypeStruct((r, d), t) for r, t in terms],
        input_output_aliases={1: 0} if chained else {},
        compiler_params=pltpu.CompilerParams(vmem_limit_bytes=VMEM_LIMIT, dimension_semantics=("arbitrary",)),
        cost_estimate=pl.CostEstimate(flops=4 * total * d * ff, bytes_accessed=4 * d * ff, transcendentals=0),
    )(jnp.stack(owners).astype(jnp.int32), *chained, *dys, *[pre] * blocks, w_down, w_in)


def dw_down_body(pieces, *refs):
    refs = refs[1:]
    pres, dys, (out, hidden, dy_all) = refs[:4], refs[4:4 + pieces], refs[4 + pieces:]

    @pl.when(pl.program_id(1) == 0)
    def _():
        at = 0
        for pre in pres:
            hidden[at:at + pre.shape[0]] = act(pre[...].astype(F32)).astype(BF16)
            at += pre.shape[0]

    at = 0
    for dy in dys:
        dy_all[at:at + dy.shape[0]] = dy[...]
        at += dy.shape[0]
    out[...] = lax.dot_general(hidden[...], dy_all[...], TN, preferred_element_type=F32).astype(BF16)


def grad_w_down(pre, owners, dys):
    rows, ff = pre.shape
    block, d = rows // len(owners), dys[0].shape[1]
    m, tn = ff // 2, TILE
    return pl.pallas_call(
        functools.partial(dw_down_body, len(dys)),
        grid_spec=pltpu.PrefetchScalarGridSpec(
            num_scalar_prefetch=1,
            grid=(ff // m, d // tn),
            in_specs=[pl.BlockSpec((block, m), functools.partial(lambda k, i, j, o: (o[k], i), k)) for k in range(len(owners))]
            + [pl.BlockSpec((v.shape[0], tn), lambda i, j, o: (0, j)) for v in dys],
            out_specs=pl.BlockSpec((m, tn), lambda i, j, o: (i, j)),
            scratch_shapes=[pltpu.VMEM((rows, m), BF16), pltpu.VMEM((rows, tn), BF16)],
        ),
        out_shape=jax.ShapeDtypeStruct((ff, d), BF16),
        compiler_params=pltpu.CompilerParams(vmem_limit_bytes=VMEM_LIMIT, dimension_semantics=("arbitrary", "arbitrary")),
        cost_estimate=pl.CostEstimate(flops=2 * rows * ff * d, bytes_accessed=2 * (rows * ff + 2 * rows * d + ff * d), transcendentals=0),
    )(jnp.stack(owners).astype(jnp.int32), *[pre] * len(owners), *dys)


def dw_in_body(columns, *refs):
    pieces = len(columns)
    xs, d_pre, (out, x_all, sems) = refs[:pieces], refs[pieces], refs[-3:]

    @pl.when(pl.program_id(0) == 0)
    def _():
        copies, at = [], 0
        for k, (x, c) in enumerate(zip(xs, columns)):
            src = x.at[:, pl.ds(c, x_all.shape[1])]
            copies.append(pltpu.make_async_copy(src, x_all.at[pl.ds(at, x.shape[0])], sems.at[k]))
            at += x.shape[0]
        for copy in copies:
            copy.start()
        for copy in copies:
            copy.wait()

    out[...] = lax.dot_general(x_all[...], d_pre[...], TN, preferred_element_type=F32).astype(BF16)


def grad_w_in(xs, d_pre, part, d, out=None):
    rows, ff = d_pre.shape
    m, tn = d // 2, TILE // 2
    columns = [part * m if x.shape[1] == d else 0 for x in xs]
    chained = [] if out is None else [out]
    return pl.pallas_call(
        functools.partial(dw_in_body, columns),
        grid=(ff // tn,),
        in_specs=[pl.BlockSpec(memory_space=pl.ANY)] * len(xs)
        + [pl.BlockSpec((rows, tn), lambda i: (0, i))]
        + [pl.BlockSpec(memory_space=pl.ANY)] * len(chained),
        out_specs=pl.BlockSpec((m, tn), lambda i: (part, i)),
        scratch_shapes=[pltpu.VMEM((rows, m), BF16), pltpu.SemaphoreType.DMA((len(xs),))],
        out_shape=jax.ShapeDtypeStruct((d, ff), BF16),
        input_output_aliases={len(xs) + 1: 0} if chained else {},
        compiler_params=pltpu.CompilerParams(vmem_limit_bytes=VMEM_LIMIT, dimension_semantics=("arbitrary",)),
        cost_estimate=pl.CostEstimate(flops=2 * rows * m * ff, bytes_accessed=2 * (rows * m + rows * ff + m * ff), transcendentals=0),
    )(*xs, d_pre, *chained)


def solution(mesh):
    n = mesh.shape["tp"]
    right = [(i, (i + 1) % n) for i in range(n)]
    left = [(i, (i - 1) % n) for i in range(n)]

    def send(a, b):
        a = lax.ppermute(a, "tp", right)
        b = lax.ppermute(b, "tp", left)
        return a, b

    def add(term, got):
        return (term + got.astype(F32)).astype(BF16)

    def step(x, dy, pre, w_in, w_down):
        me = lax.axis_index("tp")
        rows, d = x.shape
        half, m = rows // 2, d // 2
        lo, ro, own, oo = lax.rem(me + n - 1, n), lax.rem(me + 1, n), me, lax.rem(me + 2, n)

        dy_lo, dy_ro = send(dy, dy)
        top, bottom = x[:half], x[half:]
        x_lot, x_rob = send(top, bottom)
        d_pre, t0 = backward([dy], [own], pre, w_in, w_down, 2)
        dy_ot, dy_ob = send(dy_lo[:half], dy_ro[half:])
        d_pre, s, u, rest_a, rest_b = backward([dy_lo, dy_ro], [lo, ro], pre, w_in, w_down, 0, d_pre)
        s, u = send(s, u)
        x_lob, x_rot = send(bottom, top)
        x_ota, x_oba = send(x_lot[:, :m], x_rob[:, :m])
        d_pre, t3 = backward([dy_ot, dy_ob], [oo], pre, w_in, w_down, 3, d_pre)
        s, u = send(add(t3[:half], s), add(t3[half:], u))
        x_otb, x_obb = send(x_lot[:, m:], x_rob[:, m:])
        dw_down = grad_w_down(pre, [lo, ro, own, oo], [dy_lo, dy_ro, dy, dy_ot, dy_ob])
        dw_in = grad_w_in([x_lot, x_lob, x_rot, x_rob, x, x_ota, x_oba], d_pre, 0, d)
        s, u = send(add(rest_a, s), add(rest_b, u))
        dw_in = grad_w_in([x_lot, x_lob, x_rot, x_rob, x, x_otb, x_obb], d_pre, 1, d, dw_in)
        dx = jnp.concatenate([add(t0[:half], s), add(t0[half:], u)])
        return dx, dw_in, dw_down

    tokens = P(("dp", "tp"), None)
    return jax.shard_map(
        step,
        mesh=mesh,
        in_specs=(tokens, tokens, P("dp", "tp"), P(None, "tp"), P("tp", None)),
        out_specs=(tokens, P("dp", "tp"), tokens),
        check_vma=False,
    )
```

```python
import functools

import jax
import jax.numpy as jnp
from jax import lax
from jax.experimental import pallas as pl
from jax.experimental.pallas import tpu as pltpu
from jax.sharding import PartitionSpec as P

NT = (((1,), (1,)), ((), ()))
TN = (((0,), (0,)), ((), ()))
F32, BF16 = jnp.float32, jnp.bfloat16
TILE = 768
LAST = 32
MIB = 2**20


def act(pre):
    return jnp.square(jax.nn.relu(pre))


def backward_body(nd, pieces, blocks, chained, *refs):
    refs = refs[1 + chained:]
    dys, pres, (wd, wi), refs = refs[:pieces], refs[pieces:pieces + blocks], refs[pieces + blocks:pieces + blocks + 2], refs[pieces + blocks + 2:]
    dp_out, *t_out = refs[:2] if blocks == 1 else refs[:5]
    dp_all, *dy_all = refs[1 + len(t_out):]
    i = pl.program_id(0)
    rows = dp_out.shape[0] // blocks
    half = rows // 2
    tile = wd.shape[0]
    if pieces == 1:
        dy_all = dys[0]
    else:
        dy_all = dy_all[0]

        @pl.when(i == 0)
        def _():
            at = 0
            for dy in dys:
                dy_all[at:at + dy.shape[0]] = dy[...]
                at += dy.shape[0]

    @pl.when(i < nd)
    def _():
        d_hidden = lax.dot_general(dy_all[...], wd[...], NT, preferred_element_type=F32)
        for k in range(blocks):
            part = slice(k * rows, (k + 1) * rows)
            dp = (d_hidden[part] * (2.0 * jnp.maximum(pres[k][...].astype(F32), 0.0))).astype(BF16)
            dp_out[part] = dp
            dp_all[part, pl.ds(pl.multiple_of(i * tile, tile), tile)] = dp

    @pl.when(i >= nd)
    def _():
        t = lax.dot_general(dp_all[...], wi[...], NT, preferred_element_type=F32)
        if blocks == 1:
            t_out[0][...] = t
        else:
            first_a, first_b, rest_a, rest_b = t_out
            first_a[...] = t[:half].astype(BF16)
            rest_b[...] = t[half:rows]
            rest_a[...] = t[rows:rows + half]
            first_b[...] = t[rows + half:].astype(BF16)


def backward(me, dys, owners, pre, w_in, w_down, place, d_pre=None):
    chained = [] if d_pre is None else [d_pre]
    blocks = len(owners)
    total, d = sum(v.shape[0] for v in dys), dys[0].shape[1]
    rows, ff = total // blocks, pre.shape[1]
    half = rows // 2
    nd, ni = ff // TILE, d // TILE
    phase1 = lambda i: jnp.minimum(i, nd - 1)
    phase2 = lambda i: jnp.maximum(i - nd, 0)

    def pre_spec(k):
        return pl.BlockSpec((rows, TILE), lambda i, o: (lax.rem(o[0] + owners[k], pre.shape[0] // rows), phase1(i)))

    terms = [(rows, F32)] if blocks == 1 else [(half, BF16), (half, BF16), (half, F32), (half, F32)]
    return pl.pallas_call(
        functools.partial(backward_body, nd, len(dys), blocks, len(chained)),
        grid_spec=pltpu.PrefetchScalarGridSpec(
            num_scalar_prefetch=1,
            grid=(nd + ni,),
            in_specs=[pl.BlockSpec(memory_space=pl.ANY)] * len(chained)
            + [pl.BlockSpec(v.shape, lambda i, o: (0, 0)) for v in dys]
            + [pre_spec(k) for k in range(blocks)]
            + [pl.BlockSpec((TILE, d), lambda i, o: (phase1(i), 0)), pl.BlockSpec((TILE, ff), lambda i, o: (phase2(i), 0))],
            out_specs=[pl.BlockSpec((total, TILE), lambda i, o: (place, phase1(i)))]
            + [pl.BlockSpec((r, TILE), lambda i, o: (0, phase2(i))) for r, _ in terms],
            scratch_shapes=[pltpu.VMEM((total, ff), BF16)] + [pltpu.VMEM((total, d), BF16)] * (len(dys) > 1),
        ),
        out_shape=[jax.ShapeDtypeStruct((pre.shape[0], ff), BF16)] + [jax.ShapeDtypeStruct((r, d), t) for r, t in terms],
        input_output_aliases={1: 0} if chained else {},
        compiler_params=pltpu.CompilerParams(vmem_limit_bytes=(36 if blocks == 1 else 48) * MIB, dimension_semantics=("arbitrary",)),
        cost_estimate=pl.CostEstimate(flops=4 * total * d * ff, bytes_accessed=4 * d * ff, transcendentals=0),
    )(me, *chained, *dys, *[pre] * blocks, w_down, w_in)


def most_body(t, s, u, out):
    rows, size = t.shape[0], s.shape[0]
    out[:size] = (t[:size] + s[...].astype(F32)).astype(BF16)
    out[rows - size:] = (t[rows - size:] + u[...].astype(F32)).astype(BF16)


def last_body(t, s, u, _, out):
    size = s.shape[0]
    out[:size] = (t[:size] + s[...].astype(F32)).astype(BF16)
    out[size:] = (t[size:] + u[...].astype(F32)).astype(BF16)


def finish(term, s0, u0, s1, u1):
    rows, d = term.shape
    tn = d // 2
    middle = 2 * s1.shape[0]
    spec = lambda r: pl.BlockSpec((r, tn), lambda j: (0, j))
    params = pltpu.CompilerParams(vmem_limit_bytes=16 * MIB, dimension_semantics=("arbitrary",))
    dx = pl.pallas_call(
        most_body,
        grid=(d // tn,),
        in_specs=[spec(v.shape[0]) for v in (term, s0, u0)],
        out_specs=spec(rows),
        out_shape=pltpu.HBM((rows, d), BF16),
        compiler_params=params,
        cost_estimate=pl.CostEstimate(flops=rows * d, bytes_accessed=8 * rows * d, transcendentals=0),
    )(term, s0, u0)
    place = pl.BlockSpec((pl.Element(middle), pl.Element(d)), lambda i: ((rows - middle) // 2, 0))
    whole = pl.BlockSpec(s1.shape, lambda i: (0, 0))
    return pl.pallas_call(
        last_body,
        grid=(1,),
        in_specs=[place, whole, whole, pl.BlockSpec(memory_space=pl.ANY)],
        out_specs=place,
        out_shape=pltpu.HBM((rows, d), BF16),
        input_output_aliases={3: 0},
        compiler_params=params,
        cost_estimate=pl.CostEstimate(flops=middle * d, bytes_accessed=8 * middle * d, transcendentals=0),
    )(term, s1, u1, dx)


def hidden_body(pre, out):
    out[...] = act(pre[...].astype(F32)).astype(BF16).T


def hidden_transposed(pre):
    rows, ff = pre.shape
    return pl.pallas_call(
        hidden_body,
        grid=(ff // TILE,),
        in_specs=[pl.BlockSpec((rows, TILE), lambda i: (0, i))],
        out_specs=pl.BlockSpec((TILE, rows), lambda i: (i, 0)),
        out_shape=jax.ShapeDtypeStruct((ff, rows), BF16),
        compiler_params=pltpu.CompilerParams(vmem_limit_bytes=24 * MIB, dimension_semantics=("arbitrary",)),
        cost_estimate=pl.CostEstimate(flops=4 * rows * ff, bytes_accessed=4 * rows * ff, transcendentals=0),
    )(pre)


def dw_down_body(pieces, starts, hidden, *refs):
    dys, (out, dy_all) = refs[:pieces], refs[pieces:]

    @pl.when(pl.program_id(1) == 0)
    def _():
        for k, dy in enumerate(dys):
            size = dy.shape[0]
            dy_all[pl.ds(pl.multiple_of(starts(k), 16), size)] = dy[...]

    out[...] = jnp.dot(hidden[...], dy_all[...], preferred_element_type=F32).astype(BF16)


def grad_w_down(me, hidden, starts, block, dys):
    ff, rows = hidden.shape
    d = dys[0].shape[1]
    m, tn = ff // 2, d // 3

    def body(me, *refs):
        def start(k):
            owner, row = starts[k]
            return lax.rem(me[0] + owner, rows // block) * block + row

        return dw_down_body(len(dys), start, *refs)

    return pl.pallas_call(
        body,
        grid_spec=pltpu.PrefetchScalarGridSpec(
            num_scalar_prefetch=1,
            grid=(d // tn, ff // m),
            in_specs=[pl.BlockSpec((m, rows), lambda j, i, o: (i, 0))]
            + [pl.BlockSpec((v.shape[0], tn), lambda j, i, o: (0, j)) for v in dys],
            out_specs=pl.BlockSpec((m, tn), lambda j, i, o: (i, j)),
            scratch_shapes=[pltpu.VMEM((rows, tn), BF16)],
        ),
        out_shape=jax.ShapeDtypeStruct((ff, d), BF16),
        compiler_params=pltpu.CompilerParams(vmem_limit_bytes=32 * MIB, dimension_semantics=("arbitrary", "arbitrary")),
        cost_estimate=pl.CostEstimate(flops=2 * rows * ff * d, bytes_accessed=2 * (rows * ff + 2 * rows * d + ff * d), transcendentals=0),
    )(me, hidden, *dys)


def dw_in_body(columns, *refs):
    pieces = len(columns)
    xs, d_pre, (out, x_all, sems) = refs[:pieces], refs[pieces], refs[-3:]

    @pl.when(pl.program_id(0) == 0)
    def _():
        copies, at = [], 0
        for k, (x, c) in enumerate(zip(xs, columns)):
            src = x.at[:, pl.ds(c, x_all.shape[1])]
            copies.append(pltpu.make_async_copy(src, x_all.at[pl.ds(at, x.shape[0])], sems.at[k]))
            at += x.shape[0]
        for copy in copies:
            copy.start()
        for copy in copies:
            copy.wait()

    out[...] = lax.dot_general(x_all[...], d_pre[...], TN, preferred_element_type=F32).astype(BF16)


def grad_w_in(xs, d_pre, part, d, out=None):
    rows, ff = d_pre.shape
    m, tn = d // 2, TILE
    columns = [part * m if x.shape[1] == d else 0 for x in xs]
    chained = [] if out is None else [out]
    return pl.pallas_call(
        functools.partial(dw_in_body, columns),
        grid=(ff // tn,),
        in_specs=[pl.BlockSpec(memory_space=pl.ANY)] * len(xs)
        + [pl.BlockSpec((rows, tn), lambda i: (0, i))]
        + [pl.BlockSpec(memory_space=pl.ANY)] * len(chained),
        out_specs=pl.BlockSpec((m, tn), lambda i: (part, i)),
        scratch_shapes=[pltpu.VMEM((rows, m), BF16), pltpu.SemaphoreType.DMA((len(xs),))],
        out_shape=jax.ShapeDtypeStruct((d, ff), BF16),
        input_output_aliases={len(xs) + 1: 0} if chained else {},
        compiler_params=pltpu.CompilerParams(vmem_limit_bytes=26 * MIB, dimension_semantics=("arbitrary",)),
        cost_estimate=pl.CostEstimate(flops=2 * rows * m * ff, bytes_accessed=2 * (rows * m + rows * ff + m * ff), transcendentals=0),
    )(*xs, d_pre, *chained)


def solution(mesh):
    n = mesh.shape["tp"]
    right = [(i, (i + 1) % n) for i in range(n)]
    left = [(i, (i - 1) % n) for i in range(n)]

    def send(a, b):
        a = lax.ppermute(a, "tp", right)
        b = lax.ppermute(b, "tp", left)
        return a, b

    def add(term, got):
        return (term + got.astype(F32)).astype(BF16)

    def step(x, dy, pre, w_in, w_down):
        me = lax.axis_index("tp").reshape(1)
        rows, d = x.shape
        half, m = rows // 2, d // 2
        lo, ro, own, oo = n - 1, 1, 0, 2

        dy_lo, dy_ro = send(dy, dy)
        x_lot, x_rob = send(x[:half], x[half:])
        d_pre, t0 = backward(me, [dy], [own], pre, w_in, w_down, 2)
        hidden = hidden_transposed(pre)
        dy_ot, dy_ob = send(dy_lo[:half], dy_ro[half:])
        d_pre, s, u, rest_a, rest_b = backward(me, [dy_lo, dy_ro], [lo, ro], pre, w_in, w_down, 0, d_pre)
        s, u = send(s, u)
        x_lob, x_rot = send(x[half:], x[:half])
        x_ota, x_oba = send(x_lot[:, :m], x_rob[:, :m])
        d_pre, t3 = backward(me, [dy_ot, dy_ob], [oo], pre, w_in, w_down, 3, d_pre)
        s, u = send(add(t3[:half], s), add(t3[half:], u))
        x_otb, x_obb = send(x_lot[:, m:], x_rob[:, m:])
        starts = [(lo, 0), (ro, 0), (own, 0), (oo, 0), (oo, half)]
        dw_down = grad_w_down(me, hidden, starts, rows, [dy_lo, dy_ro, dy, dy_ot, dy_ob])
        dw_in = grad_w_in([x_lot, x_lob, x_rot, x_rob, x, x_ota, x_oba], d_pre, 0, d)
        c = half - LAST
        s0, u0 = send(add(rest_a[:c], s[:c]), add(rest_b[LAST:], u[LAST:]))
        s1, u1 = send(add(rest_a[c:], s[c:]), add(rest_b[:LAST], u[:LAST]))
        dw_in = grad_w_in([x_lot, x_lob, x_rot, x_rob, x, x_otb, x_obb], d_pre, 1, d, dw_in)
        dx = finish(t0, s0, u0, s1, u1)
        return dx, dw_in, dw_down

    tokens = P(("dp", "tp"), None)
    return jax.shard_map(
        step,
        mesh=mesh,
        in_specs=(tokens, tokens, P("dp", "tp"), P(None, "tp"), P("tp", None)),
        out_specs=(tokens, P("dp", "tp"), tokens),
        check_vma=False,
    )
```

```python
import functools

import jax
import jax.numpy as jnp
from jax import lax
from jax.experimental import pallas as pl
from jax.experimental.pallas import tpu as pltpu
from jax.sharding import PartitionSpec as P

NT = (((1,), (1,)), ((), ()))
TN = (((0,), (0,)), ((), ()))
F32, BF16 = jnp.float32, jnp.bfloat16
TILE = 768
LAST = 32
MIB = 2**20


def act(pre):
    return jnp.square(jax.nn.relu(pre))


def backward_body(nd, pieces, blocks, chained, *refs):
    refs = refs[1 + chained:]
    dys, pres, (wd, wi), refs = refs[:pieces], refs[pieces:pieces + blocks], refs[pieces + blocks:pieces + blocks + 2], refs[pieces + blocks + 2:]
    dp_out, *t_out = refs[:2] if blocks == 1 else refs[:5]
    dp_all, *dy_all = refs[1 + len(t_out):]
    i = pl.program_id(0)
    rows = dp_out.shape[0] // blocks
    half = rows // 2
    tile = wd.shape[0]
    if pieces == 1:
        dy_all = dys[0]
    else:
        dy_all = dy_all[0]

        @pl.when(i == 0)
        def _():
            at = 0
            for dy in dys:
                dy_all[at:at + dy.shape[0]] = dy[...]
                at += dy.shape[0]

    @pl.when(i < nd)
    def _():
        d_hidden = lax.dot_general(dy_all[...], wd[...], NT, preferred_element_type=F32)
        for k in range(blocks):
            part = slice(k * rows, (k + 1) * rows)
            pre = pres[k][...].astype(F32)
            dp = jnp.where(pre > 0, d_hidden[part] * (2.0 * pre), 0.0).astype(BF16)
            dp_out[part] = dp
            dp_all[part, pl.ds(pl.multiple_of(i * tile, tile), tile)] = dp

    @pl.when(i >= nd)
    def _():
        t = lax.dot_general(dp_all[...], wi[...], NT, preferred_element_type=F32)
        if blocks == 1:
            t_out[0][...] = t
        else:
            first_a, first_b, rest_a, rest_b = t_out
            first_a[...] = t[:half].astype(BF16)
            rest_b[...] = t[half:rows]
            rest_a[...] = t[rows:rows + half]
            first_b[...] = t[rows + half:].astype(BF16)


def backward(me, dys, owners, pre, w_in, w_down, place, d_pre=None):
    chained = [] if d_pre is None else [d_pre]
    blocks = len(owners)
    total, d = sum(v.shape[0] for v in dys), dys[0].shape[1]
    rows, ff = total // blocks, pre.shape[1]
    half = rows // 2
    nd, ni = ff // TILE, d // TILE
    phase1 = lambda i: jnp.minimum(i, nd - 1)
    phase2 = lambda i: jnp.maximum(i - nd, 0)

    def pre_spec(k):
        return pl.BlockSpec((rows, TILE), lambda i, o: (lax.rem(o[0] + owners[k], pre.shape[0] // rows), phase1(i)))

    terms = [(rows, F32)] if blocks == 1 else [(half, BF16), (half, BF16), (half, F32), (half, F32)]
    return pl.pallas_call(
        functools.partial(backward_body, nd, len(dys), blocks, len(chained)),
        grid_spec=pltpu.PrefetchScalarGridSpec(
            num_scalar_prefetch=1,
            grid=(nd + ni,),
            in_specs=[pl.BlockSpec(memory_space=pl.ANY)] * len(chained)
            + [pl.BlockSpec(v.shape, lambda i, o: (0, 0)) for v in dys]
            + [pre_spec(k) for k in range(blocks)]
            + [pl.BlockSpec((TILE, d), lambda i, o: (phase1(i), 0)), pl.BlockSpec((TILE, ff), lambda i, o: (phase2(i), 0))],
            out_specs=[pl.BlockSpec((total, TILE), lambda i, o: (place, phase1(i)))]
            + [pl.BlockSpec((r, TILE), lambda i, o: (0, phase2(i))) for r, _ in terms],
            scratch_shapes=[pltpu.VMEM((total, ff), BF16)] + [pltpu.VMEM((total, d), BF16)] * (len(dys) > 1),
        ),
        out_shape=[pltpu.HBM((pre.shape[0], ff), BF16)] + [jax.ShapeDtypeStruct((r, d), t) for r, t in terms],
        input_output_aliases={1: 0} if chained else {},
        compiler_params=pltpu.CompilerParams(vmem_limit_bytes=(36 if blocks == 1 else 48) * MIB, dimension_semantics=("arbitrary",)),
        cost_estimate=pl.CostEstimate(flops=4 * total * d * ff, bytes_accessed=4 * d * ff, transcendentals=0),
    )(me, *chained, *dys, *[pre] * blocks, w_down, w_in)


def most_body(t, s, u, out):
    rows, size = t.shape[0], s.shape[0]
    out[:size] = (t[:size] + s[...].astype(F32)).astype(BF16)
    out[rows - size:] = (t[rows - size:] + u[...].astype(F32)).astype(BF16)


def last_body(t, s, u, _, out):
    size = s.shape[0]
    out[:size] = (t[:size] + s[...].astype(F32)).astype(BF16)
    out[size:] = (t[size:] + u[...].astype(F32)).astype(BF16)


def finish(term, s0, u0, s1, u1):
    rows, d = term.shape
    tn = d // 2
    middle = 2 * s1.shape[0]
    spec = lambda r: pl.BlockSpec((r, tn), lambda j: (0, j))
    params = pltpu.CompilerParams(vmem_limit_bytes=16 * MIB, dimension_semantics=("arbitrary",))
    dx = pl.pallas_call(
        most_body,
        grid=(d // tn,),
        in_specs=[spec(v.shape[0]) for v in (term, s0, u0)],
        out_specs=spec(rows),
        out_shape=pltpu.HBM((rows, d), BF16),
        compiler_params=params,
        cost_estimate=pl.CostEstimate(flops=rows * d, bytes_accessed=8 * rows * d, transcendentals=0),
    )(term, s0, u0)
    place = pl.BlockSpec((pl.Element(middle), pl.Element(d)), lambda i: ((rows - middle) // 2, 0))
    whole = pl.BlockSpec(s1.shape, lambda i: (0, 0))
    return pl.pallas_call(
        last_body,
        grid=(1,),
        in_specs=[place, whole, whole, pl.BlockSpec(memory_space=pl.ANY)],
        out_specs=place,
        out_shape=pltpu.HBM((rows, d), BF16),
        input_output_aliases={3: 0},
        compiler_params=params,
        cost_estimate=pl.CostEstimate(flops=middle * d, bytes_accessed=8 * middle * d, transcendentals=0),
    )(term, s1, u1, dx)


def hidden_body(pre, out):
    out[...] = act(pre[...].astype(F32)).astype(BF16).T


def hidden_transposed(pre):
    rows, ff = pre.shape
    return pl.pallas_call(
        hidden_body,
        grid=(ff // TILE,),
        in_specs=[pl.BlockSpec((rows, TILE), lambda i: (0, i))],
        out_specs=pl.BlockSpec((TILE, rows), lambda i: (i, 0)),
        out_shape=pltpu.HBM((ff, rows), BF16),
        compiler_params=pltpu.CompilerParams(vmem_limit_bytes=24 * MIB, dimension_semantics=("arbitrary",)),
        cost_estimate=pl.CostEstimate(flops=4 * rows * ff, bytes_accessed=4 * rows * ff, transcendentals=0),
    )(pre)


def dw_down_body(pieces, starts, hidden, *refs):
    dys, (out, dy_all) = refs[:pieces], refs[pieces:]

    @pl.when(pl.program_id(1) == 0)
    def _():
        for k, dy in enumerate(dys):
            size = dy.shape[0]
            dy_all[pl.ds(pl.multiple_of(starts(k), 16), size)] = dy[...]

    out[...] = jnp.dot(hidden[...], dy_all[...], preferred_element_type=F32).astype(BF16)


def grad_w_down(me, hidden, starts, block, dys):
    ff, rows = hidden.shape
    d = dys[0].shape[1]
    m, tn = ff // 2, d // 3

    def body(me, *refs):
        def start(k):
            owner, row = starts[k]
            return lax.rem(me[0] + owner, rows // block) * block + row

        return dw_down_body(len(dys), start, *refs)

    return pl.pallas_call(
        body,
        grid_spec=pltpu.PrefetchScalarGridSpec(
            num_scalar_prefetch=1,
            grid=(d // tn, ff // m),
            in_specs=[pl.BlockSpec((m, rows), lambda j, i, o: (i, 0))]
            + [pl.BlockSpec((v.shape[0], tn), lambda j, i, o: (0, j)) for v in dys],
            out_specs=pl.BlockSpec((m, tn), lambda j, i, o: (i, j)),
            scratch_shapes=[pltpu.VMEM((rows, tn), BF16)],
        ),
        out_shape=jax.ShapeDtypeStruct((ff, d), BF16),
        compiler_params=pltpu.CompilerParams(vmem_limit_bytes=32 * MIB, dimension_semantics=("arbitrary", "arbitrary")),
        cost_estimate=pl.CostEstimate(flops=2 * rows * ff * d, bytes_accessed=2 * (rows * ff + 2 * rows * d + ff * d), transcendentals=0),
    )(me, hidden, *dys)


def dw_in_body(columns, *refs):
    pieces = len(columns)
    xs, d_pre, (out, x_all, sems) = refs[:pieces], refs[pieces], refs[-3:]

    @pl.when(pl.program_id(0) == 0)
    def _():
        copies, at = [], 0
        for k, (x, c) in enumerate(zip(xs, columns)):
            src = x.at[:, pl.ds(c, x_all.shape[1])]
            copies.append(pltpu.make_async_copy(src, x_all.at[pl.ds(at, x.shape[0])], sems.at[k]))
            at += x.shape[0]
        for copy in copies:
            copy.start()
        for copy in copies:
            copy.wait()

    out[...] = lax.dot_general(x_all[...], d_pre[...], TN, preferred_element_type=F32).astype(BF16)


def grad_w_in(xs, d_pre, part, d, out=None):
    rows, ff = d_pre.shape
    m, tn = d // 2, TILE
    columns = [part * m if x.shape[1] == d else 0 for x in xs]
    chained = [] if out is None else [out]
    return pl.pallas_call(
        functools.partial(dw_in_body, columns),
        grid=(ff // tn,),
        in_specs=[pl.BlockSpec(memory_space=pl.ANY)] * len(xs)
        + [pl.BlockSpec((rows, tn), lambda i: (0, i))]
        + [pl.BlockSpec(memory_space=pl.ANY)] * len(chained),
        out_specs=pl.BlockSpec((m, tn), lambda i: (part, i)),
        scratch_shapes=[pltpu.VMEM((rows, m), BF16), pltpu.SemaphoreType.DMA((len(xs),))],
        out_shape=jax.ShapeDtypeStruct((d, ff), BF16),
        input_output_aliases={len(xs) + 1: 0} if chained else {},
        compiler_params=pltpu.CompilerParams(vmem_limit_bytes=26 * MIB, dimension_semantics=("arbitrary",)),
        cost_estimate=pl.CostEstimate(flops=2 * rows * m * ff, bytes_accessed=2 * (rows * m + rows * ff + m * ff), transcendentals=0),
    )(*xs, d_pre, *chained)


def solution(mesh):
    n = mesh.shape["tp"]
    right = [(i, (i + 1) % n) for i in range(n)]
    left = [(i, (i - 1) % n) for i in range(n)]

    def send(a, b):
        a = lax.ppermute(a, "tp", right)
        b = lax.ppermute(b, "tp", left)
        return a, b

    def add(term, got):
        return (term + got.astype(F32)).astype(BF16)

    def step(x, dy, pre, w_in, w_down):
        me = lax.axis_index("tp").reshape(1)
        rows, d = x.shape
        half, m = rows // 2, d // 2
        lo, ro, own, oo = n - 1, 1, 0, 2

        dy_lo, dy_ro = send(dy, dy)
        x_lot, x_rob = send(x[:half], x[half:])
        d_pre, t0 = backward(me, [dy], [own], pre, w_in, w_down, 2)
        hidden = hidden_transposed(pre)
        dy_ot, dy_ob = send(dy_lo[:half], dy_ro[half:])
        d_pre, s, u, rest_a, rest_b = backward(me, [dy_lo, dy_ro], [lo, ro], pre, w_in, w_down, 0, d_pre)
        s, u = send(s, u)
        x_lob, x_rot = send(x[half:], x[:half])
        x_ota, x_oba = send(x_lot[:, :m], x_rob[:, :m])
        d_pre, t3 = backward(me, [dy_ot, dy_ob], [oo], pre, w_in, w_down, 3, d_pre)
        s, u = send(add(t3[:half], s), add(t3[half:], u))
        x_otb, x_obb = send(x_lot[:, m:], x_rob[:, m:])
        starts = [(lo, 0), (ro, 0), (own, 0), (oo, 0), (oo, half)]
        dw_down = grad_w_down(me, hidden, starts, rows, [dy_lo, dy_ro, dy, dy_ot, dy_ob])
        dw_in = grad_w_in([x_lot, x_lob, x_rot, x_rob, x, x_ota, x_oba], d_pre, 0, d)
        c = half - LAST
        s0, u0 = send(add(rest_a[:c], s[:c]), add(rest_b[LAST:], u[LAST:]))
        s1, u1 = send(add(rest_a[c:], s[c:]), add(rest_b[:LAST], u[:LAST]))
        dw_in = grad_w_in([x_lot, x_lob, x_rot, x_rob, x, x_otb, x_obb], d_pre, 1, d, dw_in)
        dx = finish(t0, s0, u0, s1, u1)
        return dx, dw_in, dw_down

    tokens = P(("dp", "tp"), None)
    return jax.shard_map(
        step,
        mesh=mesh,
        in_specs=(tokens, tokens, P("dp", "tp"), P(None, "tp"), P("tp", None)),
        out_specs=(tokens, P("dp", "tp"), tokens),
        check_vma=False,
    )
```

```python
import functools

import jax
import jax.numpy as jnp
from jax import lax
from jax.experimental import pallas as pl
from jax.experimental.pallas import tpu as pltpu
from jax.sharding import PartitionSpec as P

NT = (((1,), (1,)), ((), ()))
TN = (((0,), (0,)), ((), ()))
F32, BF16 = jnp.float32, jnp.bfloat16
TILE = 768
LAST = 24
MIB = 2**20


def act(pre):
    return jnp.square(jax.nn.relu(pre))


def backward_body(nd, pieces, blocks, chained, *refs):
    refs = refs[1 + chained:]
    dys, pres, (wd, wi), refs = refs[:pieces], refs[pieces:pieces + blocks], refs[pieces + blocks:pieces + blocks + 2], refs[pieces + blocks + 2:]
    dp_out, *t_out = refs[:2] if blocks == 1 else refs[:5]
    dp_all, *dy_all = refs[1 + len(t_out):]
    i = pl.program_id(0)
    rows = dp_out.shape[0] // blocks
    half = rows // 2
    tile = wd.shape[0]
    if pieces == 1:
        dy_all = dys[0]
    else:
        dy_all = dy_all[0]

        @pl.when(i == 0)
        def _():
            at = 0
            for dy in dys:
                dy_all[at:at + dy.shape[0]] = dy[...]
                at += dy.shape[0]

    @pl.when(i < nd)
    def _():
        d_hidden = lax.dot_general(dy_all[...], wd[...], NT, preferred_element_type=F32)
        for k in range(blocks):
            part = slice(k * rows, (k + 1) * rows)
            pre = pres[k][...].astype(F32)
            dp = jnp.where(pre > 0, d_hidden[part] * (2.0 * pre), 0.0).astype(BF16)
            dp_out[part] = dp
            dp_all[part, pl.ds(pl.multiple_of(i * tile, tile), tile)] = dp

    @pl.when(i >= nd)
    def _():
        t = lax.dot_general(dp_all[...], wi[...], NT, preferred_element_type=F32)
        if blocks == 1:
            t_out[0][...] = t
        else:
            first_a, first_b, rest_a, rest_b = t_out
            first_a[...] = t[:half].astype(BF16)
            rest_b[...] = t[half:rows]
            rest_a[...] = t[rows:rows + half]
            first_b[...] = t[rows + half:].astype(BF16)


def backward(me, dys, owners, pre, w_in, w_down, place, d_pre=None):
    chained = [] if d_pre is None else [d_pre]
    blocks = len(owners)
    total, d = sum(v.shape[0] for v in dys), dys[0].shape[1]
    rows, ff = total // blocks, pre.shape[1]
    half = rows // 2
    nd, ni = ff // TILE, d // TILE
    phase1 = lambda i: jnp.minimum(i, nd - 1)
    phase2 = lambda i: jnp.maximum(i - nd, 0)

    def pre_spec(k):
        return pl.BlockSpec((rows, TILE), lambda i, o: (lax.rem(o[0] + owners[k], pre.shape[0] // rows), phase1(i)))

    terms = [(rows, F32)] if blocks == 1 else [(half, BF16), (half, BF16), (half, F32), (half, F32)]
    return pl.pallas_call(
        functools.partial(backward_body, nd, len(dys), blocks, len(chained)),
        grid_spec=pltpu.PrefetchScalarGridSpec(
            num_scalar_prefetch=1,
            grid=(nd + ni,),
            in_specs=[pl.BlockSpec(memory_space=pl.ANY)] * len(chained)
            + [pl.BlockSpec(v.shape, lambda i, o: (0, 0)) for v in dys]
            + [pre_spec(k) for k in range(blocks)]
            + [pl.BlockSpec((TILE, d), lambda i, o: (phase1(i), 0)), pl.BlockSpec((TILE, ff), lambda i, o: (phase2(i), 0))],
            out_specs=[pl.BlockSpec((total, TILE), lambda i, o: (place, phase1(i)))]
            + [pl.BlockSpec((r, TILE), lambda i, o: (0, phase2(i))) for r, _ in terms],
            scratch_shapes=[pltpu.VMEM((total, ff), BF16)] + [pltpu.VMEM((total, d), BF16)] * (len(dys) > 1),
        ),
        out_shape=[pltpu.HBM((pre.shape[0], ff), BF16)] + [jax.ShapeDtypeStruct((r, d), t) for r, t in terms],
        input_output_aliases={1: 0} if chained else {},
        compiler_params=pltpu.CompilerParams(vmem_limit_bytes=(36 if blocks == 1 else 48) * MIB, dimension_semantics=("arbitrary",)),
        cost_estimate=pl.CostEstimate(flops=4 * total * d * ff, bytes_accessed=4 * d * ff, transcendentals=0),
    )(me, *chained, *dys, *[pre] * blocks, w_down, w_in)


def most_body(t, s, u, out):
    rows, size = t.shape[0], s.shape[0]
    out[:size] = (t[:size] + s[...].astype(F32)).astype(BF16)
    out[rows - size:] = (t[rows - size:] + u[...].astype(F32)).astype(BF16)


def last_body(t, s, u, _, out):
    size = s.shape[0]
    out[:size] = (t[:size] + s[...].astype(F32)).astype(BF16)
    out[size:] = (t[size:] + u[...].astype(F32)).astype(BF16)


def finish(term, s0, u0, s1, u1):
    rows, d = term.shape
    tn = d // 2
    middle = 2 * s1.shape[0]
    spec = lambda r: pl.BlockSpec((r, tn), lambda j: (0, j))
    params = pltpu.CompilerParams(vmem_limit_bytes=16 * MIB, dimension_semantics=("arbitrary",))
    dx = pl.pallas_call(
        most_body,
        grid=(d // tn,),
        in_specs=[spec(v.shape[0]) for v in (term, s0, u0)],
        out_specs=spec(rows),
        out_shape=pltpu.HBM((rows, d), BF16),
        compiler_params=params,
        cost_estimate=pl.CostEstimate(flops=rows * d, bytes_accessed=8 * rows * d, transcendentals=0),
    )(term, s0, u0)
    place = pl.BlockSpec((pl.Element(middle), pl.Element(d)), lambda i: ((rows - middle) // 2, 0))
    whole = pl.BlockSpec(s1.shape, lambda i: (0, 0))
    return pl.pallas_call(
        last_body,
        grid=(1,),
        in_specs=[place, whole, whole, pl.BlockSpec(memory_space=pl.ANY)],
        out_specs=place,
        out_shape=pltpu.HBM((rows, d), BF16),
        input_output_aliases={3: 0},
        compiler_params=params,
        cost_estimate=pl.CostEstimate(flops=middle * d, bytes_accessed=8 * middle * d, transcendentals=0),
    )(term, s1, u1, dx)


def hidden_body(pre, out):
    out[...] = act(pre[...].astype(F32)).astype(BF16).T


def hidden_transposed(pre):
    rows, ff = pre.shape
    return pl.pallas_call(
        hidden_body,
        grid=(ff // TILE,),
        in_specs=[pl.BlockSpec((rows, TILE), lambda i: (0, i))],
        out_specs=pl.BlockSpec((TILE, rows), lambda i: (i, 0)),
        out_shape=pltpu.HBM((ff, rows), BF16),
        compiler_params=pltpu.CompilerParams(vmem_limit_bytes=58 * MIB, dimension_semantics=("arbitrary",)),
        cost_estimate=pl.CostEstimate(flops=4 * rows * ff, bytes_accessed=4 * rows * ff, transcendentals=0),
    )(pre)


def dw_down_body(pieces, starts, hidden, *refs):
    dys, (out, dy_all) = refs[:pieces], refs[pieces:]

    @pl.when(pl.program_id(1) == 0)
    def _():
        for k, dy in enumerate(dys):
            size = dy.shape[0]
            dy_all[pl.ds(pl.multiple_of(starts(k), 16), size)] = dy[...]

    out[...] = jnp.dot(hidden[...], dy_all[...], preferred_element_type=F32).astype(BF16)


def grad_w_down(me, hidden, starts, block, dys):
    ff, rows = hidden.shape
    d = dys[0].shape[1]
    m, tn = ff // 2, d // 3

    def body(me, *refs):
        def start(k):
            owner, row = starts[k]
            return lax.rem(me[0] + owner, rows // block) * block + row

        return dw_down_body(len(dys), start, *refs)

    return pl.pallas_call(
        body,
        grid_spec=pltpu.PrefetchScalarGridSpec(
            num_scalar_prefetch=1,
            grid=(d // tn, ff // m),
            in_specs=[pl.BlockSpec((m, rows), lambda j, i, o: (i, 0))]
            + [pl.BlockSpec((v.shape[0], tn), lambda j, i, o: (0, j)) for v in dys],
            out_specs=pl.BlockSpec((m, tn), lambda j, i, o: (i, j)),
            scratch_shapes=[pltpu.VMEM((rows, tn), BF16)],
        ),
        out_shape=jax.ShapeDtypeStruct((ff, d), BF16),
        compiler_params=pltpu.CompilerParams(vmem_limit_bytes=58 * MIB, dimension_semantics=("arbitrary", "arbitrary")),
        cost_estimate=pl.CostEstimate(flops=2 * rows * ff * d, bytes_accessed=2 * (rows * ff + 2 * rows * d + ff * d), transcendentals=0),
    )(me, hidden, *dys)


def dw_in_body(columns, *refs):
    pieces = len(columns)
    xs, d_pre, (out, x_all, sems) = refs[:pieces], refs[pieces], refs[-3:]

    @pl.when(pl.program_id(0) == 0)
    def _():
        copies, at = [], 0
        for k, (x, c) in enumerate(zip(xs, columns)):
            src = x.at[:, pl.ds(c, x_all.shape[1])]
            copies.append(pltpu.make_async_copy(src, x_all.at[pl.ds(at, x.shape[0])], sems.at[k]))
            at += x.shape[0]
        for copy in copies:
            copy.start()
        for copy in copies:
            copy.wait()

    out[...] = lax.dot_general(x_all[...], d_pre[...], TN, preferred_element_type=F32).astype(BF16)


def grad_w_in(xs, d_pre, part, d, out=None):
    rows, ff = d_pre.shape
    m, tn = d // 2, TILE
    columns = [part * m if x.shape[1] == d else 0 for x in xs]
    chained = [] if out is None else [out]
    return pl.pallas_call(
        functools.partial(dw_in_body, columns),
        grid=(ff // tn,),
        in_specs=[pl.BlockSpec(memory_space=pl.ANY)] * len(xs)
        + [pl.BlockSpec((rows, tn), lambda i: (0, i))]
        + [pl.BlockSpec(memory_space=pl.ANY)] * len(chained),
        out_specs=pl.BlockSpec((m, tn), lambda i: (part, i)),
        scratch_shapes=[pltpu.VMEM((rows, m), BF16), pltpu.SemaphoreType.DMA((len(xs),))],
        out_shape=jax.ShapeDtypeStruct((d, ff), BF16),
        input_output_aliases={len(xs) + 1: 0} if chained else {},
        compiler_params=pltpu.CompilerParams(vmem_limit_bytes=26 * MIB, dimension_semantics=("arbitrary",)),
        cost_estimate=pl.CostEstimate(flops=2 * rows * m * ff, bytes_accessed=2 * (rows * m + rows * ff + m * ff), transcendentals=0),
    )(*xs, d_pre, *chained)


def solution(mesh):
    n = mesh.shape["tp"]
    right = [(i, (i + 1) % n) for i in range(n)]
    left = [(i, (i - 1) % n) for i in range(n)]

    def send(a, b):
        a = lax.ppermute(a, "tp", right)
        b = lax.ppermute(b, "tp", left)
        return a, b

    def add(term, got):
        return (term + got.astype(F32)).astype(BF16)

    def step(x, dy, pre, w_in, w_down):
        me = lax.axis_index("tp").reshape(1)
        rows, d = x.shape
        half, m = rows // 2, d // 2
        lo, ro, own, oo = n - 1, 1, 0, 2

        dy_lo, dy_ro = send(dy, dy)
        x_lot, x_rob = send(x[:half], x[half:])
        d_pre, t0 = backward(me, [dy], [own], pre, w_in, w_down, 2)
        hidden = hidden_transposed(pre)
        dy_ot, dy_ob = send(dy_lo[:half], dy_ro[half:])
        d_pre, s, u, rest_a, rest_b = backward(me, [dy_lo, dy_ro], [lo, ro], pre, w_in, w_down, 0, d_pre)
        s, u = send(s, u)
        x_lob, x_rot = send(x[half:], x[:half])
        x_ota, x_oba = send(x_lot[:, :m], x_rob[:, :m])
        d_pre, t3 = backward(me, [dy_ot, dy_ob], [oo], pre, w_in, w_down, 3, d_pre)
        s, u = send(add(t3[:half], s), add(t3[half:], u))
        x_otb, x_obb = send(x_lot[:, m:], x_rob[:, m:])
        starts = [(lo, 0), (ro, 0), (own, 0), (oo, 0), (oo, half)]
        dw_down = grad_w_down(me, hidden, starts, rows, [dy_lo, dy_ro, dy, dy_ot, dy_ob])
        dw_in = grad_w_in([x_lot, x_lob, x_rot, x_rob, x, x_ota, x_oba], d_pre, 0, d)
        c = half - LAST
        s0, u0 = send(add(rest_a[:c], s[:c]), add(rest_b[LAST:], u[LAST:]))
        s1, u1 = send(add(rest_a[c:], s[c:]), add(rest_b[:LAST], u[:LAST]))
        dw_in = grad_w_in([x_lot, x_lob, x_rot, x_rob, x, x_otb, x_obb], d_pre, 1, d, dw_in)
        dx = finish(t0, s0, u0, s1, u1)
        return dx, dw_in, dw_down

    tokens = P(("dp", "tp"), None)
    return jax.shard_map(
        step,
        mesh=mesh,
        in_specs=(tokens, tokens, P("dp", "tp"), P(None, "tp"), P("tp", None)),
        out_specs=(tokens, P("dp", "tp"), tokens),
        check_vma=False,
    )
```

```python
import functools

import jax
import jax.numpy as jnp
from jax import lax
from jax.experimental import pallas as pl
from jax.experimental.pallas import tpu as pltpu
from jax.sharding import PartitionSpec as P

NT = (((1,), (1,)), ((), ()))
TN = (((0,), (0,)), ((), ()))
F32, BF16 = jnp.float32, jnp.bfloat16
TILE = 768
LAST = 24
MIB = 2**20


def act(pre):
    return jnp.square(jax.nn.relu(pre))


def backward_body(nd, pieces, blocks, chained, *refs):
    refs = refs[1 + chained:]
    dys, pres, (wd, wi), refs = refs[:pieces], refs[pieces:pieces + blocks], refs[pieces + blocks:pieces + blocks + 2], refs[pieces + blocks + 2:]
    dp_out, *t_out = refs[:2] if blocks == 1 else refs[:5]
    dp_all, *dy_all = refs[1 + len(t_out):]
    i = pl.program_id(0)
    rows = dp_out.shape[0] // blocks
    half = rows // 2
    tile = wd.shape[0]
    if pieces == 1:
        dy_all = dys[0]
    else:
        dy_all = dy_all[0]

        @pl.when(i == 0)
        def _():
            at = 0
            for dy in dys:
                dy_all[at:at + dy.shape[0]] = dy[...]
                at += dy.shape[0]

    @pl.when(i < nd)
    def _():
        d_hidden = lax.dot_general(dy_all[...], wd[...], NT, preferred_element_type=F32)
        for k in range(blocks):
            part = slice(k * rows, (k + 1) * rows)
            pre = pres[k][...].astype(F32)
            dp = jnp.where(pre > 0, d_hidden[part] * (2.0 * pre), 0.0).astype(BF16)
            dp_out[part] = dp
            dp_all[part, pl.ds(pl.multiple_of(i * tile, tile), tile)] = dp

    @pl.when(i >= nd)
    def _():
        t = lax.dot_general(dp_all[...], wi[...], NT, preferred_element_type=F32)
        if blocks == 1:
            t_out[0][...] = t
        else:
            first_a, first_b, rest_a, rest_b = t_out
            first_a[...] = t[:half].astype(BF16)
            rest_b[...] = t[half:rows]
            rest_a[...] = t[rows:rows + half]
            first_b[...] = t[rows + half:].astype(BF16)


def backward(me, dys, owners, pre, w_in, w_down, place, d_pre=None):
    chained = [] if d_pre is None else [d_pre]
    blocks = len(owners)
    total, d = sum(v.shape[0] for v in dys), dys[0].shape[1]
    rows, ff = total // blocks, pre.shape[1]
    half = rows // 2
    nd, ni = ff // TILE, d // TILE
    phase1 = lambda i: jnp.minimum(i, nd - 1)
    phase2 = lambda i: jnp.maximum(i - nd, 0)

    def pre_spec(k):
        return pl.BlockSpec((rows, TILE), lambda i, o: (lax.rem(o[0] + owners[k], pre.shape[0] // rows), phase1(i)))

    terms = [(rows, F32)] if blocks == 1 else [(half, BF16), (half, BF16), (half, F32), (half, F32)]
    return pl.pallas_call(
        functools.partial(backward_body, nd, len(dys), blocks, len(chained)),
        grid_spec=pltpu.PrefetchScalarGridSpec(
            num_scalar_prefetch=1,
            grid=(nd + ni,),
            in_specs=[pl.BlockSpec(memory_space=pl.ANY)] * len(chained)
            + [pl.BlockSpec(v.shape, lambda i, o: (0, 0)) for v in dys]
            + [pre_spec(k) for k in range(blocks)]
            + [pl.BlockSpec((TILE, d), lambda i, o: (phase1(i), 0)), pl.BlockSpec((TILE, ff), lambda i, o: (phase2(i), 0))],
            out_specs=[pl.BlockSpec((total, TILE), lambda i, o: (place, phase1(i)))]
            + [pl.BlockSpec((r, TILE), lambda i, o: (0, phase2(i))) for r, _ in terms],
            scratch_shapes=[pltpu.VMEM((total, ff), BF16)] + [pltpu.VMEM((total, d), BF16)] * (len(dys) > 1),
        ),
        out_shape=[pltpu.HBM((pre.shape[0], ff), BF16)] + [jax.ShapeDtypeStruct((r, d), t) for r, t in terms],
        input_output_aliases={1: 0} if chained else {},
        compiler_params=pltpu.CompilerParams(vmem_limit_bytes=(32 if blocks == 1 else 44) * MIB, dimension_semantics=("arbitrary",)),
        cost_estimate=pl.CostEstimate(flops=4 * total * d * ff, bytes_accessed=4 * d * ff, transcendentals=0),
    )(me, *chained, *dys, *[pre] * blocks, w_down, w_in)


def most_body(t, s, u, out):
    rows, size = t.shape[0], s.shape[0]
    out[:size] = (t[:size] + s[...].astype(F32)).astype(BF16)
    out[rows - size:] = (t[rows - size:] + u[...].astype(F32)).astype(BF16)


def last_body(t, s, u, _, out):
    size = s.shape[0]
    out[:size] = (t[:size] + s[...].astype(F32)).astype(BF16)
    out[size:] = (t[size:] + u[...].astype(F32)).astype(BF16)


def finish(term, s0, u0, s1, u1):
    rows, d = term.shape
    tn = d // 2
    middle = 2 * s1.shape[0]
    spec = lambda r: pl.BlockSpec((r, tn), lambda j: (0, j))
    params = pltpu.CompilerParams(vmem_limit_bytes=10 * MIB, dimension_semantics=("arbitrary",))
    dx = pl.pallas_call(
        most_body,
        grid=(d // tn,),
        in_specs=[spec(v.shape[0]) for v in (term, s0, u0)],
        out_specs=spec(rows),
        out_shape=pltpu.HBM((rows, d), BF16),
        compiler_params=params,
        cost_estimate=pl.CostEstimate(flops=rows * d, bytes_accessed=8 * rows * d, transcendentals=0),
    )(term, s0, u0)
    place = pl.BlockSpec((pl.Element(middle), pl.Element(d)), lambda i: ((rows - middle) // 2, 0))
    whole = pl.BlockSpec(s1.shape, lambda i: (0, 0))
    return pl.pallas_call(
        last_body,
        grid=(1,),
        in_specs=[place, whole, whole, pl.BlockSpec(memory_space=pl.ANY)],
        out_specs=place,
        out_shape=pltpu.HBM((rows, d), BF16),
        input_output_aliases={3: 0},
        compiler_params=params,
        cost_estimate=pl.CostEstimate(flops=middle * d, bytes_accessed=8 * middle * d, transcendentals=0),
    )(term, s1, u1, dx)


def hidden_body(pre, out):
    out[...] = act(pre[...].astype(F32)).astype(BF16).T


def hidden_transposed(pre):
    rows, ff = pre.shape
    return pl.pallas_call(
        hidden_body,
        grid=(ff // TILE,),
        in_specs=[pl.BlockSpec((rows, TILE), lambda i: (0, i))],
        out_specs=pl.BlockSpec((TILE, rows), lambda i: (i, 0)),
        out_shape=pltpu.HBM((ff, rows), BF16),
        compiler_params=pltpu.CompilerParams(vmem_limit_bytes=20 * MIB, dimension_semantics=("arbitrary",)),
        cost_estimate=pl.CostEstimate(flops=4 * rows * ff, bytes_accessed=4 * rows * ff, transcendentals=0),
    )(pre)


def dw_down_body(pieces, starts, hidden, *refs):
    dys, (out, dy_all) = refs[:pieces], refs[pieces:]

    @pl.when(pl.program_id(1) == 0)
    def _():
        for k, dy in enumerate(dys):
            size = dy.shape[0]
            dy_all[pl.ds(pl.multiple_of(starts(k), 16), size)] = dy[...]

    out[...] = jnp.dot(hidden[...], dy_all[...], preferred_element_type=F32).astype(BF16)


def grad_w_down(me, hidden, starts, block, dys):
    ff, rows = hidden.shape
    d = dys[0].shape[1]
    m, tn = ff // 2, d // 3

    def body(me, *refs):
        def start(k):
            owner, row = starts[k]
            return lax.rem(me[0] + owner, rows // block) * block + row

        return dw_down_body(len(dys), start, *refs)

    return pl.pallas_call(
        body,
        grid_spec=pltpu.PrefetchScalarGridSpec(
            num_scalar_prefetch=1,
            grid=(d // tn, ff // m),
            in_specs=[pl.BlockSpec((m, rows), lambda j, i, o: (i, 0))]
            + [pl.BlockSpec((v.shape[0], tn), lambda j, i, o: (0, j)) for v in dys],
            out_specs=pl.BlockSpec((m, tn), lambda j, i, o: (i, j)),
            scratch_shapes=[pltpu.VMEM((rows, tn), BF16)],
        ),
        out_shape=jax.ShapeDtypeStruct((ff, d), BF16),
        compiler_params=pltpu.CompilerParams(vmem_limit_bytes=28 * MIB, dimension_semantics=("arbitrary", "arbitrary")),
        cost_estimate=pl.CostEstimate(flops=2 * rows * ff * d, bytes_accessed=2 * (rows * ff + 2 * rows * d + ff * d), transcendentals=0),
    )(me, hidden, *dys)


def dw_in_body(columns, *refs):
    pieces = len(columns)
    xs, d_pre, (out, x_all, sems) = refs[:pieces], refs[pieces], refs[-3:]

    @pl.when(pl.program_id(0) == 0)
    def _():
        copies, at = [], 0
        for k, (x, c) in enumerate(zip(xs, columns)):
            src = x.at[:, pl.ds(c, x_all.shape[1])]
            copies.append(pltpu.make_async_copy(src, x_all.at[pl.ds(at, x.shape[0])], sems.at[k]))
            at += x.shape[0]
        for copy in copies:
            copy.start()
        for copy in copies:
            copy.wait()

    out[...] = lax.dot_general(x_all[...], d_pre[...], TN, preferred_element_type=F32).astype(BF16)


def grad_w_in(xs, d_pre, part, d, out=None):
    rows, ff = d_pre.shape
    m, tn = d // 2, TILE
    columns = [part * m if x.shape[1] == d else 0 for x in xs]
    chained = [] if out is None else [out]
    return pl.pallas_call(
        functools.partial(dw_in_body, columns),
        grid=(ff // tn,),
        in_specs=[pl.BlockSpec(memory_space=pl.ANY)] * len(xs)
        + [pl.BlockSpec((rows, tn), lambda i: (0, i))]
        + [pl.BlockSpec(memory_space=pl.ANY)] * len(chained),
        out_specs=pl.BlockSpec((m, tn), lambda i: (part, i)),
        scratch_shapes=[pltpu.VMEM((rows, m), BF16), pltpu.SemaphoreType.DMA((len(xs),))],
        out_shape=jax.ShapeDtypeStruct((d, ff), BF16),
        input_output_aliases={len(xs) + 1: 0} if chained else {},
        compiler_params=pltpu.CompilerParams(vmem_limit_bytes=22 * MIB, dimension_semantics=("arbitrary",)),
        cost_estimate=pl.CostEstimate(flops=2 * rows * m * ff, bytes_accessed=2 * (rows * m + rows * ff + m * ff), transcendentals=0),
    )(*xs, d_pre, *chained)


def solution(mesh):
    n = mesh.shape["tp"]
    right = [(i, (i + 1) % n) for i in range(n)]
    left = [(i, (i - 1) % n) for i in range(n)]

    def send(a, b):
        a = lax.ppermute(a, "tp", right)
        b = lax.ppermute(b, "tp", left)
        return a, b

    def add(term, got):
        return (term + got.astype(F32)).astype(BF16)

    def step(x, dy, pre, w_in, w_down):
        me = lax.axis_index("tp").reshape(1)
        rows, d = x.shape
        half, m = rows // 2, d // 2
        lo, ro, own, oo = n - 1, 1, 0, 2

        dy_lo, dy_ro = send(dy, dy)
        x_lot, x_rob = send(x[:half], x[half:])
        d_pre, t0 = backward(me, [dy], [own], pre, w_in, w_down, 2)
        hidden = hidden_transposed(pre)
        dy_ot, dy_ob = send(dy_lo[:half], dy_ro[half:])
        d_pre, s, u, rest_a, rest_b = backward(me, [dy_lo, dy_ro], [lo, ro], pre, w_in, w_down, 0, d_pre)
        s, u = send(s, u)
        x_lob, x_rot = send(x[half:], x[:half])
        x_ota, x_oba = send(x_lot[:, :m], x_rob[:, :m])
        d_pre, t3 = backward(me, [dy_ot, dy_ob], [oo], pre, w_in, w_down, 3, d_pre)
        s, u = send(add(t3[:half], s), add(t3[half:], u))
        x_otb, x_obb = send(x_lot[:, m:], x_rob[:, m:])
        starts = [(lo, 0), (ro, 0), (own, 0), (oo, 0), (oo, half)]
        dw_down = grad_w_down(me, hidden, starts, rows, [dy_lo, dy_ro, dy, dy_ot, dy_ob])
        dw_in = grad_w_in([x_lot, x_lob, x_rot, x_rob, x, x_ota, x_oba], d_pre, 0, d)
        c = half - LAST
        s0, u0 = send(add(rest_a[:c], s[:c]), add(rest_b[LAST:], u[LAST:]))
        s1, u1 = send(add(rest_a[c:], s[c:]), add(rest_b[:LAST], u[:LAST]))
        dw_in = grad_w_in([x_lot, x_lob, x_rot, x_rob, x, x_otb, x_obb], d_pre, 1, d, dw_in)
        dx = finish(t0, s0, u0, s1, u1)
        return dx, dw_in, dw_down

    tokens = P(("dp", "tp"), None)
    return jax.shard_map(
        step,
        mesh=mesh,
        in_specs=(tokens, tokens, P("dp", "tp"), P(None, "tp"), P("tp", None)),
        out_specs=(tokens, P("dp", "tp"), tokens),
        check_vma=False,
    )
```
